32 devices in a mesh: dp: 2 (over y), expert: 4 (over z), tile: 4 (over x, core).
Axes of the slice: x: 2, y: 2, z: 4, core: 2. Of those that a mesh axis runs over, the one named last changes fastest.
Arguments:
- tokens: bfloat16 [512, 4096], P(('dp', 'expert'), 'tile'), may hold values from -6 to 6
- hidden: bfloat16 [512, 2, 7168], P(('dp', 'expert'), None, 'tile'), may hold values from -6 to 6
- routes: int32 [512, 2], P(('dp', 'expert')), may hold values from 0 to 3, all different within a row; in each aligned block of 64 rows (0 to 63, 64 to 127, ...) at most 40 rows name the same one
- lengths: int32 [8], P(('dp', 'expert')), may hold values from 1 to 64, as said below
Outputs:
- hessian_in: float32 [4, 4096, 4096], P('expert', 'tile', 'dp')
- hessian_down: float32 [4, 7168, 7168], P('expert', 'tile', 'dp')
The draws below stay inside these ranges and needn't reach their ends.
Inputs may be any that keep to these rules, and one draw needn't show every extreme that they name: `routes`: in each aligned block of 64 rows (the rows of one group) no expert is named by more than 40 rows, a bound that some block reaches. The live rows of group g are its first lengths[g] rows; the last group is full.
All inputs are finite; a program needn't handle non-finite values.
Results may differ from the reference program's by a relative error of at most 0.0003.
Values may be sent and summed in bfloat16 or wider, within the bound.
No kernel may reach another device: no remote copies, remote signals or barrier semaphores. Data moves between devices by JAX's collectives and lax.ppermute only.
A program may use at most 128 MiB of HBM per device.

```python
import math
import jax
import jax.numpy as jnp
import numpy as np
from jax import lax

D = 4096
FFW = 7168
TOP = 2
TOK_DEV = 64
EXPERTS = 4
GROUPS = 8
TOKENS = 512
CAP = 40


def draw_lengths(key, part):
    group_index = jnp.arange(GROUPS, dtype=jnp.int32)
    lowest = TOK_DEV // 3
    rising = lowest + (TOK_DEV - lowest) * group_index // max(GROUPS - 1, 1)
    jitter = jax.random.randint(key, (GROUPS,), 0, max(TOK_DEV // 8, 1), dtype=jnp.int32)
    jitter = jnp.where(group_index == GROUPS - 1, 0, jitter)
    return jnp.maximum(rising - jitter, 1).astype(jnp.int32)


def steps_of(stream_key, dims, shards, low, top_value):
    gain = 1.0
    for axis_at, parts in shards:
        heights = jax.random.uniform(jax.random.fold_in(jax.random.fold_in(stream_key, 6), axis_at), (parts,), jnp.float32, low / len(shards), top_value / len(shards))
        gain = gain * jnp.repeat(jnp.exp(heights), dims[axis_at] // parts).reshape((-1,) + (1,) * (len(dims) - 1 - axis_at))
    return gain


def assign_block(own_key, own, number, rows, number_of, top, bound, slope):
    order = jax.random.permutation(own_key, number_of)
    crowded, ordinary = portions_of(number_of, rows * top, bound, slope, True), portions_of(number_of, rows * top, bound, slope, False)
    places = jnp.arange(number_of)

    def named(sizes, rotation):
        used = int((sizes > 0).sum())
        fixed = max(1, used // 4)
        passed = fixed + (places - fixed + rotation * (used - fixed)) % max(1, number_of - fixed)
        return jnp.zeros((number_of,), jnp.int32).at[order[jnp.where(places < fixed, places, passed)]].set(jnp.asarray(sizes, jnp.int32))

    sizes = jnp.where(number % 4 == 0, named(crowded, number // 4), named(ordinary, number - number // 4 - 1))
    mixed = jax.random.permutation(jax.random.fold_in(own, 3), number_of)
    source_of, receiver = mixed[0:number_of // 2 * 2:2], mixed[1:number_of // 2 * 2:2]
    room = jnp.minimum(sizes[source_of] - 1, bound - sizes[receiver]) // 2
    room = jnp.where((source_of == order[0]) | (receiver == order[0]) | (sizes[receiver] == 0), 0, jnp.maximum(room, 0))
    passed = jax.random.randint(jax.random.fold_in(own, 4), (number_of // 2,), 0, 1 << 20) % (room + 1)
    sizes = sizes.at[source_of].add(-passed).at[receiver].add(passed)
    members = jnp.searchsorted(jnp.cumsum(sizes), jnp.arange(rows * top), side="right").astype(jnp.int32)
    grid = members.reshape(top, rows).T
    grid = grid[jax.random.permutation(jax.random.fold_in(own, 1), rows)]
    rotation = jax.random.randint(jax.random.fold_in(own, 2), (rows, 1), 0, top)
    return jnp.take_along_axis(grid, (jnp.arange(top)[None, :] + rotation) % top, axis=1)


def portions_of(count, total, limit, slope, full):
    loads = [(1 << 20) // math.isqrt(rank ** slope) + 1 for rank in range(1, count + 1)]
    largest = limit if full else min(limit, max(-(-total // count), total * loads[0] // sum(loads)))
    least = 1 if total - largest >= count - 1 else 0
    counts, spare = [largest] + [least] * (count - 1), total - largest - least * (count - 1)
    while spare > 0:
        candidates = [i for i in range(1, count) if counts[i] < largest] or [i for i in range(1, count) if counts[i] < limit]
        pool, budget = sum([loads[i] for i in candidates]), spare
        for i in candidates:
            addition = min(limit - counts[i], max(1, budget * loads[i] // pool), spare)
            counts[i] = counts[i] + addition
            spare = spare - addition
    return np.array(counts)


def gaussian(key, shape, spread, reach, pieces=(), kind=jnp.bfloat16):
    drawn = jax.random.normal(key, shape, jnp.float32) * spread
    if len(pieces) > 0:
        drawn = steps_of(key, shape, pieces, -0.22, 0.18) * drawn
    return jnp.clip(drawn, min=-reach, max=reach).astype(kind)


def setup_inputs(seed: int = 0) -> dict:
    streams_of = jax.random.split(jax.random.key(seed), 5)
    tokens = gaussian(streams_of[0], (TOKENS, D), 1.0, 6.0, ((0, 8), (1, 4)))
    hidden = gaussian(streams_of[1], (TOKENS, TOP, FFW), 1.0, 6.0, ((0, 8), (2, 4)))
    routes_keys = jax.random.split(jax.random.fold_in(streams_of[2], 1), TOKENS // TOK_DEV)
    routes_turns = jax.random.permutation(jax.random.fold_in(streams_of[2], 3), TOKENS // TOK_DEV)
    routes = jax.vmap(lambda own, number: assign_block(jax.random.fold_in(streams_of[2], 2), own, number, TOK_DEV, EXPERTS, TOP, CAP, 1))(routes_keys, routes_turns).reshape((TOKENS, TOP))
    lengths = draw_lengths(jax.random.fold_in(streams_of[4], 71), 0)
    return dict(tokens=tokens, hidden=hidden, routes=routes, lengths=lengths)


def reference(tokens, hidden, routes, lengths):
    token_total = tokens.shape[0]
    token_index = jnp.arange(token_total, dtype=jnp.int32)
    live_mask = (token_index % TOK_DEV) < lengths[token_index // TOK_DEV]
    row_limit = GROUPS * CAP

    def one_expert(expert):
        picked = (routes == expert) & live_mask[:, None]
        token_hit = jnp.any(picked, axis=1)
        pair_count = jnp.sum(picked.astype(jnp.float32))
        ordering = jnp.argsort(jnp.where(token_hit, 0, 1).astype(jnp.int32), stable=True)[:row_limit]
        chosen = tokens[ordering] * token_hit[ordering][:, None].astype(jnp.bfloat16)
        weights = picked[ordering].astype(jnp.float32)
        chosen_hidden = jnp.sum(hidden[ordering].astype(jnp.float32) * weights[:, :, None], axis=1).astype(jnp.bfloat16)
        factor = jnp.float32(2.0) / jnp.maximum(pair_count, jnp.float32(1.0))
        gram_tokens = jnp.dot(chosen.T, chosen, preferred_element_type=jnp.float32) * factor
        gram_hidden = jnp.dot(chosen_hidden.T, chosen_hidden, preferred_element_type=jnp.float32) * factor
        return gram_tokens, gram_hidden

    hessian_in, hessian_down = lax.map(one_expert, jnp.arange(EXPERTS, dtype=jnp.int32))
    return hessian_in, hessian_down
```

```python
import jax
import jax.numpy as jnp
from jax import lax
from jax.sharding import PartitionSpec as P


def broadcast(value, axis, source):
    kept = jnp.where(lax.axis_index(axis) == source, value, 0).astype(value.dtype)
    return lax.psum(kept, axis)


def contract(left, right):
    return lax.dot_general(
        left, right, (((0,), (0,)), ((), ())), preferred_element_type=jnp.float32
    )


def dispatch_tables(routes, live_count, experts, share_size, senders):
    token_count = routes.shape[0]
    top_count = routes.shape[1]
    flat_routes = routes.reshape(token_count * top_count)
    pair_index = jnp.arange(token_count * top_count, dtype=jnp.int32)
    pair_live = pair_index // top_count < live_count
    expert_ids = jnp.arange(experts, dtype=jnp.int32)
    onehot = ((flat_routes[:, None] == expert_ids[None, :]) & pair_live[:, None]).astype(
        jnp.float32
    )
    before = jnp.cumsum(onehot, axis=0) - onehot
    position = jnp.sum(before * onehot, axis=1).astype(jnp.int32)
    target = (
        position // share_size * (experts * share_size)
        + flat_routes * share_size
        + position % share_size
    )
    slot_total = senders * experts * share_size
    placed = (target[None, :] == jnp.arange(slot_total, dtype=jnp.int32)[:, None]) & pair_live[
        None, :
    ]
    return (placed.astype(jnp.float32), jnp.sum(onehot, axis=0))


def on_device(tokens, hidden, routes, lengths):
    experts = lax.axis_size("expert")
    senders = lax.axis_size("dp")
    tiles = lax.axis_size("tile")
    token_count = tokens.shape[0]
    top_count = routes.shape[1]
    share_size = (5 * token_count + 2 * experts * senders - 1) // (2 * experts * senders)
    placed, local_counts = dispatch_tables(routes, lengths[0], experts, share_size, senders)
    slot_total = placed.shape[0]
    by_token = jnp.sum(placed.reshape(slot_total, token_count, top_count), axis=2).astype(
        jnp.bfloat16
    )
    send_tokens = jnp.dot(by_token, tokens, preferred_element_type=jnp.float32).astype(jnp.bfloat16)
    flat_hidden = hidden.reshape(token_count * top_count, hidden.shape[2])
    send_hidden = jnp.dot(
        placed.astype(jnp.bfloat16), flat_hidden, preferred_element_type=jnp.float32
    ).astype(jnp.bfloat16)
    slot_tokens, slot_hidden = (
        lax.all_to_all(send_tokens, ("dp", "expert"), split_axis=0, concat_axis=0, tiled=True),
        lax.all_to_all(send_hidden, ("dp", "expert"), split_axis=0, concat_axis=0, tiled=True),
    )
    global_counts = lax.psum(local_counts, ("dp", "expert"))
    own_expert = lax.axis_index("expert")
    own_count = jnp.sum(
        jnp.where(jnp.arange(experts, dtype=jnp.int32) == own_expert, global_counts, 0.0)
    )
    factor = 2.0 / jnp.maximum(own_count, 1.0)
    all_tokens, all_hidden = (
        lax.all_gather(slot_tokens, "dp", axis=0, tiled=True),
        lax.all_gather(slot_hidden, "dp", axis=0, tiled=True),
    )
    width_tokens = slot_tokens.shape[1] * tiles // senders
    width_hidden = slot_hidden.shape[1] * tiles // senders
    group_index = lax.axis_index("dp")
    if senders % tiles == 0:
        source_tile = group_index * tiles // senders
        offset_tokens = group_index * width_tokens - source_tile * slot_tokens.shape[1]
        offset_hidden = group_index * width_hidden - source_tile * slot_hidden.shape[1]
        own_tokens = lax.dynamic_slice_in_dim(all_tokens, offset_tokens, width_tokens, 1)
        own_hidden = lax.dynamic_slice_in_dim(all_hidden, offset_hidden, width_hidden, 1)
        joined = jnp.concatenate([own_tokens, own_hidden], axis=1)
        arrived = broadcast(joined, "tile", source_tile)
        column_tokens = arrived[:, :width_tokens]
        column_hidden = arrived[:, width_tokens:]
    else:
        wide_tokens, wide_hidden = (
            lax.all_gather(all_tokens, "tile", axis=1, tiled=True),
            lax.all_gather(all_hidden, "tile", axis=1, tiled=True),
        )
        column_tokens = lax.dynamic_slice_in_dim(
            wide_tokens, group_index * width_tokens, width_tokens, 1
        )
        column_hidden = lax.dynamic_slice_in_dim(
            wide_hidden, group_index * width_hidden, width_hidden, 1
        )
    gram_tokens = contract(all_tokens, column_tokens)
    gram_hidden = contract(all_hidden, column_hidden)
    return ((gram_tokens * factor)[None], (gram_hidden * factor)[None])


def pair_swap(count):
    return [(i, i ^ 1) for i in range(count)]


def pack_tables(routes, live_count, experts, own_expert, capacity):
    token_count, top_count = routes.shape
    flat_routes = routes.reshape(token_count * top_count)
    pair_index = jnp.arange(token_count * top_count, dtype=jnp.int32)
    pair_live = pair_index // top_count < live_count
    relative = flat_routes - own_expert
    relative = jnp.where(relative < 0, relative + experts, relative)
    expert_ids = jnp.arange(experts, dtype=jnp.int32)
    onehot = ((relative[:, None] == expert_ids[None, :]) & pair_live[:, None]).astype(jnp.float32)
    before = jnp.cumsum(onehot, axis=0) - onehot
    position = jnp.sum(before * onehot, axis=1).astype(jnp.int32)
    target = relative * capacity + position
    slots = jnp.arange(experts * capacity, dtype=jnp.int32)
    placed = (target[None, :] == slots[:, None]) & pair_live[None, :]
    return placed.astype(jnp.float32), jnp.sum(onehot, axis=0)


def in_plane(tokens, hidden, routes, lengths):
    experts = lax.axis_size("expert")
    senders = lax.axis_size("dp")
    tiles = lax.axis_size("tile")
    token_count = tokens.shape[0]
    top_count = routes.shape[1]
    wide = tiles // senders
    capacity = senders * ((5 * token_count + 2 * experts * senders - 1) // (2 * experts * senders))
    own_expert = lax.axis_index("expert")
    own_sender = lax.axis_index("dp")
    own_tile = lax.axis_index("tile")
    inside = own_tile // wide == own_sender
    even = own_tile % wide == 0

    def plane_index(sender, half, core):
        return sender * tiles + half * wide + core

    cores = range(wide)
    across = [(plane_index(s, s, c), plane_index(s, 1 - s, c)) for s in range(senders) for c in cores]
    diagonal = [
        (plane_index(s, 1 - s, c), plane_index(1 - s, s, c)) for s in range(senders) for c in cores
    ]

    def to_sender(value):
        return lax.ppermute(value, "dp", pair_swap(senders))

    def to_half(value):
        return lax.ppermute(value, ("dp", "tile"), across)

    def to_corner(value):
        return lax.ppermute(value, ("dp", "tile"), diagonal)

    def to_core(value):
        return lax.ppermute(value, "tile", pair_swap(tiles))

    def to_expert(value, shift):
        return lax.ppermute(value, "expert", [(i, (i + shift) % experts) for i in range(experts)])

    placed, counts = pack_tables(routes, lengths[0], experts, own_expert, capacity)
    slot_total = placed.shape[0]
    by_token = jnp.sum(placed.reshape(slot_total, token_count, top_count), axis=2).astype(jnp.bfloat16)
    send_tokens = jnp.dot(by_token, tokens, preferred_element_type=jnp.float32).astype(jnp.bfloat16)
    flat_hidden = hidden.reshape(token_count * top_count, hidden.shape[2])
    send_hidden = jnp.dot(
        placed.astype(jnp.bfloat16), flat_hidden, preferred_element_type=jnp.float32
    ).astype(jnp.bfloat16)
    width = tokens.shape[1]

    own = jnp.concatenate([send_tokens[:capacity], send_hidden[:capacity]], axis=1)
    total = counts[0]
    for shift in range(1, experts):
        total = total + to_expert(counts[shift:shift + 1], shift)[0]
    total = total + to_sender(total[None])[0]
    factor = 2.0 / jnp.maximum(total, 1.0)

    rest_hidden = jnp.concatenate(
        [to_expert(send_hidden[k * capacity:(k + 1) * capacity], k) for k in range(1, experts)], axis=0)
    rest_tokens = jnp.concatenate(
        [to_expert(send_tokens[k * capacity:(k + 1) * capacity], k) for k in range(1, experts)], axis=0)

    def exchange(piece, direct):
        beside = to_sender(piece)
        same = to_half(piece)
        corner = to_corner(piece) if direct else to_half(beside)
        return beside, jnp.where(inside, piece, same), jnp.where(inside, beside, corner)

    own_beside, own_first, own_second = exchange(own, True)
    h_beside, h_first, h_second = exchange(rest_hidden, False)
    t_beside, t_first, t_second = exchange(rest_tokens, True)

    def gram(own_part, rest, beside, first, second):
        left = jnp.concatenate([own_part(own), rest, own_part(own_beside), beside], axis=0)
        mine = jnp.concatenate([own_part(own_first), first, own_part(own_second), second], axis=0)
        other = to_core(mine)
        low = jnp.where(even, mine, other)
        high = jnp.where(even, other, mine)
        right = jnp.concatenate([low, high], axis=1)
        return (contract(left, right) * factor)[None]

    gram_hidden = gram(lambda v: v[:, width:], rest_hidden, h_beside, h_first, h_second)
    gram_tokens = gram(lambda v: v[:, :width], rest_tokens, t_beside, t_first, t_second)
    return gram_tokens, gram_hidden


def solution(mesh):
    pairs = mesh.shape["dp"] == 2 and mesh.shape["tile"] == 2 * mesh.shape["dp"]
    placed = (
        P(("dp", "expert"), "tile"),
        P(("dp", "expert"), None, "tile"),
        P(("dp", "expert"), None),
        P(("dp", "expert")),
    )
    return jax.shard_map(
        in_plane if pairs else on_device,
        mesh=mesh,
        in_specs=placed,
        out_specs=(P("expert", "tile", "dp"), P("expert", "tile", "dp")),
        check_vma=False,
    )
```
